128 devices in a mesh: row: 16 (over z_lo, y, core), col: 8 (over x, z_hi).
Axes of the slice: x: 4, y: 4, z: 4 (z_hi: 2, z_lo: 2; z = z_hi * 2 + z_lo), core: 2. Of those that a mesh axis runs over, the one named last changes fastest.
Arguments:
- features: bfloat16 [262144, 256], P(('row', 'col')), may hold values from -6 to 6
- tiles: bfloat16 [16, 8, 768, 128, 128], P('row', 'col'), as said below
- tile_rows: int32 [16, 8, 768], P('row', 'col'), may hold values from 0 to 127
- tile_cols: int32 [16, 8, 768], P('row', 'col'), may hold values from 0 to 255
- valid: int32 [16, 8, 768], P('row', 'col'), may hold values from 0 to 1, as said below
- weight: bfloat16 [256, 256], replicated, may hold values from -0.375 to 0.375
- bias: float32 [256], replicated, may hold values from -3 to 3
Outputs:
- hidden: bfloat16 [262144, 256], P(('row', 'col'))
The draws below stay inside these ranges and needn't reach their ends.
Inputs may be any that keep to these rules, and one draw needn't show every extreme that they name: Each cell holds between 96 and 384 valid slots at any positions; in every draw some cell has exactly 384 valid slots. `tiles`: tile entries are non-negative.
All inputs are finite; a program needn't handle non-finite values.
Results may differ from the reference program's by a relative error of at most 0.0039.
Values may be sent and summed in bfloat16 or wider, within the bound.
A program may use at most 256 MiB of HBM per device.

```python
import jax
import jax.numpy as jnp
from jax import lax

F = 256
TILE = 128
SUB = 2048
TPD = 768
NODES = 262144
N_ROW = 16
N_COL = 8


def draw_tiles(key, part):
    shape = (N_ROW, N_COL, TPD, TILE, TILE)
    spread = (SUB / (TPD * TILE * TILE)) ** 0.5
    values = jnp.minimum(jnp.abs(jax.random.normal(key, shape, jnp.float32)) * spread, 5.0 * spread)
    return values.astype(jnp.bfloat16)


def draw_valid(key, part):
    subkeys = jax.random.split(key, 3)
    cells = N_ROW * N_COL
    shifts = jax.random.randint(subkeys[0], (cells,), 1, 4)
    counts = jnp.right_shift(jnp.full((cells,), TPD, jnp.int32), shifts)
    chosen = jax.random.randint(subkeys[1], (), 0, cells)
    counts = jnp.where(jnp.arange(cells) == chosen, TPD // 2, counts)
    orders = jax.vmap(lambda sub_key: jax.random.permutation(sub_key, TPD))(jax.random.split(subkeys[2], cells))
    valid_flags = (orders < counts[:, None]).astype(jnp.int32)
    return valid_flags.reshape(N_ROW, N_COL, TPD)


def touch_ends(values, own_key, smallest, high):
    shape = values.shape
    index_at = [jax.random.randint(jax.random.fold_in(own_key, axis), (), 0, shape[axis]) for axis in range(len(shape))]
    values = values.at[tuple(index_at)].set(smallest)
    longest = shape.index(max(shape))
    index_at[longest] = (index_at[longest] + 1) % shape[longest]
    return values.at[tuple(index_at)].set(high)


def block_scale(rng, dims, cuts, least, high):
    factor_of, own = 1.0, jax.random.fold_in(rng, 6)
    for dim, shards_of in cuts:
        heights = jnp.exp(jax.random.uniform(jax.random.fold_in(own, dim), (shards_of,), jnp.float32, least / len(cuts), high / len(cuts)))
        factor_of = factor_of * jnp.repeat(heights, dims[dim] // shards_of).reshape([-1 if axis == dim else 1 for axis in range(len(dims))])
    return factor_of


def gaussian(key, extent, scale, limit, pieces=(), kind=jnp.bfloat16):
    entries = jax.random.normal(key, extent, jnp.float32) * scale
    if len(pieces) > 0:
        entries = block_scale(key, extent, pieces, -0.22, 0.18) * entries
    return jnp.clip(entries, min=-limit, max=limit).astype(kind)


def setup_inputs(seed: int = 0) -> dict:
    key_list = jax.random.split(jax.random.key(seed), 8)
    features = gaussian(key_list[0], (NODES, F), 1.0, 6.0, ((0, 128),))
    tiles = draw_tiles(jax.random.fold_in(key_list[7], 71), 0)
    tile_rows = touch_ends(jax.random.randint(key_list[2], (N_ROW, N_COL, TPD), 0, SUB * N_COL // TILE), jax.random.fold_in(key_list[2], 1), 0, (SUB * N_COL // TILE) - 1).astype(jnp.int32)
    tile_cols = touch_ends(jax.random.randint(key_list[3], (N_ROW, N_COL, TPD), 0, SUB * N_ROW // TILE), jax.random.fold_in(key_list[3], 1), 0, (SUB * N_ROW // TILE) - 1).astype(jnp.int32)
    valid = draw_valid(jax.random.fold_in(key_list[7], 71), 0)
    weight = gaussian(key_list[5], (F, F), F ** -0.5, 0.375)
    bias = gaussian(key_list[6], (F,), 0.5, 3.0, (), jnp.float32)
    return {"features": features, "tiles": tiles, "tile_rows": tile_rows, "tile_cols": tile_cols, "valid": valid, "weight": weight, "bias": bias}


def reference(features, tiles, tile_rows, tile_cols, valid, weight, bias):
    row_tiles = SUB * N_COL // TILE
    grouped = features.reshape(N_ROW, N_COL, SUB, F)
    flat_tiles = tiles.reshape(N_ROW * N_COL, TPD, TILE, TILE)
    flat_rows = tile_rows.reshape(N_ROW * N_COL, TPD)
    flat_cols = tile_cols.reshape(N_ROW * N_COL, TPD)
    flat_valid = valid.reshape(N_ROW * N_COL, TPD)

    def one_cell(device):
        column = device % N_COL
        panel = jnp.take(grouped, column, axis=1).reshape(-1, TILE, F)
        chosen = panel[flat_cols[device]]
        products = jnp.einsum("bij,bjf->bif", flat_tiles[device].astype(jnp.float32), chosen.astype(jnp.float32))
        products = products * flat_valid[device].astype(jnp.float32)[:, None, None]
        partial_sum = jnp.zeros((row_tiles, TILE, F), jnp.float32)
        return partial_sum.at[flat_rows[device]].add(products)

    partials = lax.map(one_cell, jnp.arange(N_ROW * N_COL, dtype=jnp.int32))
    totals = jnp.sum(partials.reshape(N_ROW, N_COL, row_tiles, TILE, F), axis=1)
    aggregated = totals.reshape(N_ROW * N_COL * SUB, F).astype(jnp.bfloat16)
    mixed = jnp.dot(aggregated, weight, preferred_element_type=jnp.float32) + bias
    return jnp.maximum(mixed, 0.0).astype(jnp.bfloat16)
```

```python
import functools

import jax
import jax.numpy as jnp
from jax import lax
from jax.experimental import pallas as pl
from jax.experimental.pallas import tpu as pltpu
from jax.sharding import PartitionSpec as P

MESH = pl.DeviceIdType.MESH
Y, ZL, CORE, X, ZH = 4, 2, 2, 4, 2
UNROLL = 8
FORWARD = ((0, 0, 0), (0, 0, 1), (0, 1, 1), (-1, 0, 0), (-1, 1, 1))
BACKWARD = ((0, 0, 1), (0, 0, 0), (0, 1, 0), (1, 0, 1), (1, 1, 0))
ACROSS = ((0, 0, 1), (0, 0, 0), (-1, 0, 0), (1, 0, 1))
LANDED = (
    tuple((dy - 1, dz, up) for dy, dz, up in FORWARD)
    + tuple((dy + 1, dz, up) for dy, dz, up in BACKWARD)
    + tuple((dy, 1 - dz, up) for dy, dz, up in ACROSS)
)


def tables(rows, cols, valid, row_tiles, pairs):
    slots = rows.shape[0]
    ids = jnp.arange(slots, dtype=jnp.int32)
    key = jnp.where(valid > 0, rows, row_tiles)
    earlier = (key[:, None] == key[None, :]) & (ids[None, :] < ids[:, None])
    rank = jnp.sum(earlier.astype(jnp.int32), axis=1)
    row_ids = jnp.arange(row_tiles, dtype=jnp.int32)
    in_row = row_ids[:, None] == key[None, :]
    count = jnp.sum(in_row.astype(jnp.int32), axis=1)
    used = (count + 1) >> 1
    start = jnp.sum(jnp.where(row_ids[None, :] < row_ids[:, None], used[None, :], 0), axis=1)
    place = jnp.sum(jnp.where(in_row, 2 * start[:, None], 0), axis=0) + rank
    place = jnp.where(valid > 0, place, -1)
    at = place[None, :] == jnp.arange(2 * pairs, dtype=jnp.int32)[:, None]
    slot = jnp.sum(jnp.where(at, ids[None, :] - slots, 0), axis=1) + slots
    col = jnp.sum(jnp.where(at, cols[None, :], 0), axis=1)
    pair_ids = jnp.arange(pairs, dtype=jnp.int32)
    first = jnp.any((start[None, :] == pair_ids[:, None]) & (count > 0)[None, :], axis=1)
    keep = jnp.where(first, 0.0, 1.0).astype(jnp.float32)
    last = jnp.where(count > 0, start + used - 1, pairs)
    return slot, col, keep, last


def kernel(
    slots, pairs, row_tiles, block,
    slot, col, keep, last, features, tiles, weight, bias, out,
    tile_store, panel_a, panel_b, sums, part_a, got_a, got_b, agg_a, agg_b,
    own_sem, tile_sem, ring_send, ring_recv, twin_send, twin_recv, sum_send, sum_recv,
):
    half = block // 2
    row, column = lax.axis_index("row"), lax.axis_index("col")
    zl, y, core = row // (Y * CORE), (row // CORE) % Y, row % CORE
    x, zh = column // ZH, column % ZH

    def at_row(dy, dz, dc=0):
        return ((zl + dz) % ZL) * (Y * CORE) + ((y + dy + Y) % Y) * CORE + (core + dc) % CORE

    def at_column(dx, dz):
        return ((x + dx + X) % X) * ZH + (zh + dz) % ZH

    up_y, down_y = (at_row(1, 0), column), (at_row(-1, 0), column)
    other_z, twin = (at_row(0, 1), column), (at_row(0, 0, 1), column)
    up_x, down_x = (row, at_column(1, 0)), (row, at_column(-1, 0))
    far_z = (row, at_column(0, 1))

    panels, gots, aggs = (panel_a, panel_b), (got_a, got_b), (agg_a, agg_b)
    parts = (part_a, panel_a)

    def load_own(h):
        return pltpu.make_async_copy(
            features.at[:, :, pl.ds(h * 128, 128)],
            panels[h].at[pl.ds(row * block, block)],
            own_sem.at[h],
        )

    load_own(0).start()
    load_own(1).start()
    group = slots // tile_sem.shape[0]
    tile_loads = [
        pltpu.make_async_copy(
            tiles.at[pl.ds(i * group, group)], tile_store.at[pl.ds(i * group, group)], tile_sem.at[i]
        )
        for i in range(tile_sem.shape[0])
    ]
    barrier = pltpu.get_barrier_semaphore()
    peers = (up_y, down_y, other_z, twin, up_x, down_x, far_z)
    for peer in peers:
        pl.semaphore_signal(barrier, inc=1, device_id=peer, device_id_type=MESH)
    pl.semaphore_wait(barrier, len(peers))

    def piece(h, spot):
        dy, dz, up = spot
        return panels[h].at[pl.ds(at_row(dy, dz) * block + up * half, half)]

    def ring_copies(h):
        copies = []
        for target, spots in ((up_y, FORWARD), (down_y, BACKWARD), (other_z, ACROSS)):
            for spot in spots:
                k = len(copies)
                copies.append(
                    pltpu.make_async_remote_copy(
                        piece(h, spot), piece(h, spot), ring_send.at[h, k], ring_recv.at[h, k],
                        device_id=target, device_id_type=MESH,
                    )
                )
        return copies

    def twin_copies(h):
        return [
            pltpu.make_async_remote_copy(
                piece(h, spot), piece(h, spot), twin_send.at[h, k], twin_recv.at[h, k],
                device_id=twin, device_id_type=MESH,
            )
            for k, spot in enumerate(LANDED + ((0, 0, 0), (0, 0, 1)))
        ]

    ring = (ring_copies(0), ring_copies(1))
    sibling = (twin_copies(0), twin_copies(1))

    def gather_start(h):
        load_own(h).wait()
        for k in (0, 5, 10, 1, 6, 11):
            ring[h][k].start()
        sibling[h][14].start()
        sibling[h][15].start()

    def gather_step(h, k, then=()):
        ring[h][k].wait_recv()
        for k_next in then:
            ring[h][k_next].start()
        sibling[h][k].start()

    def gather_first(h):
        gather_step(h, 10, (2,))
        gather_step(h, 0, (3, 12))
        gather_step(h, 5, (8, 13))
        gather_step(h, 11, (7,))
        gather_step(h, 1)
        gather_step(h, 6)

    def gather_second(h):
        gather_step(h, 2, (4,))
        gather_step(h, 7, (9,))

    def gather_rest(h):
        for k in (12, 13, 3, 8, 4, 9):
            gather_step(h, k)
        for copy in sibling[h]:
            copy.wait_recv()

    def products(h, low, high, total):
        panel = panels[h]

        def body(i, total):
            for j in range(UNROLL):
                s = i * UNROLL + j
                left = jnp.concatenate([tile_store[slot[2 * s]], tile_store[slot[2 * s + 1]]], axis=1)
                right = jnp.concatenate([panel[col[2 * s]], panel[col[2 * s + 1]]], axis=0)
                total = total * keep[s] + jnp.dot(left, right, preferred_element_type=jnp.float32)
                sums[s] = total.astype(jnp.bfloat16)
            return total

        return lax.fori_loop(low // UNROLL, high // UNROLL, body, total)

    def collect(h):
        part = parts[h]

        def body(i, carry):
            for j in range(8):
                r = i * 8 + j
                part[r] = sums[last[r]]
            return carry

        lax.fori_loop(0, row_tiles // 8, body, 0)

    def spot(dx, dz, up):
        return pl.ds(at_column(dx, dz) * block + up * half, half)

    def sum_copies(h):
        copies = []
        for dz in (1, 0):
            for target, spots in (
                (up_x, ((2, dz, 0), (1, dz, 1), (1, dz, 0))),
                (down_x, ((2, dz, 1), (-1, dz, 0), (-1, dz, 1))),
            ):
                copies += [(target, s) for s in spots]
        copies += [(far_z, (0, 1, 0)), (far_z, (0, 1, 1))]
        return [
            pltpu.make_async_remote_copy(
                parts[h].at[spot(*s)], gots[h].at[k], sum_send.at[h, k], sum_recv.at[h, k],
                device_id=target, device_id_type=MESH,
            )
            for k, (target, s) in enumerate(copies)
        ]

    adds = (sum_copies(0), sum_copies(1))

    def wide(value):
        return value.astype(jnp.float32)

    def sum_start(h, i):
        for k in (0, 3, 1, 4):
            adds[h][6 * i + k].start()

    def sum_pass(h, i):
        part, got, dz = parts[h], gots[h], 1 - i
        for k, dx, up, k_next in ((0, 1, 0, 2), (3, -1, 1, 5)):
            adds[h][6 * i + k].wait_recv()
            here = spot(dx, dz, up)
            part[here] = (wide(part[here]) + wide(got[6 * i + k])).astype(jnp.bfloat16)
            adds[h][6 * i + k_next].start()

    def sum_across(h):
        part, got = parts[h], gots[h]
        for up, ks in ((0, (2, 4)), (1, (1, 5))):
            for k in ks:
                adds[h][k].wait_recv()
            here = spot(0, 1, up)
            part[here] = (wide(part[here]) + wide(got[ks[0]]) + wide(got[ks[1]])).astype(jnp.bfloat16)
            adds[h][12 + up].start()

    def sum_end(h):
        part, got, agg = parts[h], gots[h], aggs[h]
        for up, ks in ((1, (7, 11, 13)), (0, (8, 10, 12))):
            for k in ks:
                adds[h][k].wait_recv()
            total = wide(part[spot(0, 0, up)])
            for k in ks:
                total = total + wide(got[k])
            agg[pl.ds(up * half, half)] = total.astype(jnp.bfloat16)

    zero = jnp.zeros((128, 128), jnp.float32)
    gather_start(0)
    for copy in tile_loads:
        copy.start()
    tile_store[slots] = zero.astype(jnp.bfloat16)
    sums[pairs] = zero.astype(jnp.bfloat16)
    gather_first(0)
    gather_second(0)
    gather_start(1)
    gather_rest(0)
    for copy in tile_loads:
        copy.wait()
    products(0, 0, pairs, zero)
    collect(0)
    sum_start(0, 0)
    gather_first(1)
    sum_pass(0, 0)
    sum_start(0, 1)
    gather_second(1)
    gather_rest(1)
    sum_across(0)
    for copy in ring[0] + sibling[0]:
        copy.wait_send()
    total = products(1, 0, pairs // 2, zero)
    sum_pass(0, 1)
    products(1, pairs // 2, pairs, total)
    collect(1)
    sum_start(1, 0)
    sum_end(0)
    sum_pass(1, 0)
    sum_start(1, 1)
    sum_across(1)
    sum_pass(1, 1)
    sum_end(1)

    def finish(t, carry):
        mixed = jnp.dot(
            jnp.concatenate([agg_a[t], agg_b[t]], axis=1), weight[...], preferred_element_type=jnp.float32
        )
        out[t] = jnp.maximum(mixed + bias[...], 0.0).astype(jnp.bfloat16)
        return carry

    lax.fori_loop(0, block, finish, 0)
    for copy in ring[1] + sibling[1] + adds[0] + adds[1]:
        copy.wait_send()


def on_device(features, tiles, tile_rows, tile_cols, valid, weight, bias):
    sub_rows, width = features.shape
    size, slots = tiles.shape[3], tiles.shape[2]
    block = sub_rows // size
    row_tiles = block * X * ZH
    panel_tiles = block * Y * ZL * CORE
    pairs = (slots // 2 + row_tiles) // 2
    slot, col, keep, last = tables(tile_rows[0, 0], tile_cols[0, 0], valid[0, 0], row_tiles, pairs)
    smem, vmem = pl.BlockSpec(memory_space=pltpu.SMEM), pl.BlockSpec(memory_space=pltpu.VMEM)
    hbm = pl.BlockSpec(memory_space=pl.ANY)
    dma = pltpu.SemaphoreType.DMA

    def store(*shape):
        return pltpu.VMEM(shape + (size, size), jnp.bfloat16)

    hidden = pl.pallas_call(
        functools.partial(kernel, slots, pairs, row_tiles, block),
        name="graph_layer",
        out_shape=jax.ShapeDtypeStruct((block, size, width), jnp.bfloat16),
        in_specs=[smem, smem, smem, smem, hbm, hbm, vmem, vmem],
        out_specs=vmem,
        scratch_shapes=[
            store(slots + 1), store(panel_tiles), store(panel_tiles), store(pairs + 1), store(row_tiles),
            store(14, block // 2), store(14, block // 2), store(block), store(block),
            dma((2,)), dma((8,)), dma((2, 14)), dma((2, 14)), dma((2, 16)), dma((2, 16)), dma((2, 14)), dma((2, 14)),
        ],
        compiler_params=pltpu.CompilerParams(
            collective_id=0, has_side_effects=True, vmem_limit_bytes=67043328
        ),
    )(
        slot, col, keep, last,
        features.reshape(block, size, width), tiles.reshape(slots, size, size), weight, bias.reshape(1, width),
    )
    return hidden.reshape(sub_rows, width)


def solution(mesh):
    return jax.shard_map(
        on_device,
        mesh=mesh,
        in_specs=(
            P(("row", "col"), None),
            P("row", "col", None, None, None),
            P("row", "col", None),
            P("row", "col", None),
            P("row", "col", None),
            P(),
            P(),
        ),
        out_specs=P(("row", "col"), None),
        check_vma=False,
    )
```

```python
import functools

import jax
import jax.numpy as jnp
from jax import lax
from jax.experimental import pallas as pl
from jax.experimental.pallas import tpu as pltpu
from jax.sharding import PartitionSpec as P

MESH = pl.DeviceIdType.MESH
Y, ZL, CORE, X, ZH = 4, 2, 2, 4, 2
CHUNKS = 4
UNROLL = 16
FORWARD = ((0, 0, 0), (0, 0, 1), (0, 1, 1), (-1, 0, 0), (-1, 1, 1))
BACKWARD = ((0, 0, 1), (0, 0, 0), (0, 1, 0), (1, 0, 1), (1, 1, 0))
ACROSS = ((0, 0, 1), (0, 0, 0), (-1, 0, 0), (1, 0, 1))
LANDED = (
    tuple((dy - 1, dz, up) for dy, dz, up in FORWARD)
    + tuple((dy + 1, dz, up) for dy, dz, up in BACKWARD)
    + tuple((dy, 1 - dz, up) for dy, dz, up in ACROSS)
)


def tables(rows, cols, valid, row_tiles, pairs, block):
    slots = rows.shape[0]
    ids = jnp.arange(slots, dtype=jnp.int32)
    key = jnp.where(valid > 0, rows, row_tiles)
    earlier = (key[:, None] == key[None, :]) & (ids[None, :] < ids[:, None])
    rank = jnp.sum(earlier.astype(jnp.int32), axis=1)
    row_ids = jnp.arange(row_tiles, dtype=jnp.int32)
    in_row = row_ids[:, None] == key[None, :]
    count = jnp.sum(in_row.astype(jnp.int32), axis=1)
    used = (count + 1) >> 1
    start = jnp.sum(jnp.where(row_ids[None, :] < row_ids[:, None], used[None, :], 0), axis=1)
    place = jnp.sum(jnp.where(in_row, 2 * start[:, None], 0), axis=0) + rank
    place = jnp.where(valid > 0, place, -1)
    at = place[None, :] == jnp.arange(2 * pairs, dtype=jnp.int32)[:, None]
    slot = jnp.sum(jnp.where(at, ids[None, :] - slots, 0), axis=1) + slots
    col = jnp.sum(jnp.where(at, cols[None, :], 0), axis=1)
    pair_ids = jnp.arange(pairs, dtype=jnp.int32)
    first = jnp.any((start[None, :] == pair_ids[:, None]) & (count > 0)[None, :], axis=1)
    keep = jnp.where(first, 0.0, 1.0).astype(jnp.float32)
    last = jnp.where(count > 0, start + used - 1, pairs)
    packed = (col // block) * (block // 2) + col % (block // 2)
    side = (col % block) // (block // 2)
    return slot, packed, side, keep, last


def kernel(
    slots, pairs, row_tiles, block,
    slot, col, side, keep, last, features, tiles, out,
    tile_store, panel_0, panel_1, panel_2, panel_3, sums, part_a, got_0, got_1, got_2, got_3, agg, sides,
    own_sem, tile_sem, ring_send, ring_recv, twin_send, twin_recv, sum_send, sum_recv,
):
    packs = block // 2
    half = packs // 2
    row, column = lax.axis_index("row"), lax.axis_index("col")
    zl, y, core = row // (Y * CORE), (row // CORE) % Y, row % CORE
    x, zh = column // ZH, column % ZH

    def at_row(dy, dz, dc=0):
        return ((zl + dz) % ZL) * (Y * CORE) + ((y + dy + Y) % Y) * CORE + (core + dc) % CORE

    def at_column(dx, dz):
        return ((x + dx + X) % X) * ZH + (zh + dz) % ZH

    up_y, down_y = (at_row(1, 0), column), (at_row(-1, 0), column)
    other_z, twin = (at_row(0, 1), column), (at_row(0, 0, 1), column)
    up_x, down_x = (row, at_column(1, 0)), (row, at_column(-1, 0))
    far_z = (row, at_column(0, 1))

    panels, gots = (panel_0, panel_1, panel_2, panel_3), (got_0, got_1, got_2, got_3)
    parts = ((part_a, 0), (part_a, row_tiles // 2), (panel_0, 0), (panel_1, 0))

    own = pltpu.make_async_copy(features, out, own_sem)
    own.start()
    barrier = pltpu.get_barrier_semaphore()
    peers = (up_y, down_y, other_z, twin, up_x, down_x, far_z)
    for peer in peers:
        pl.semaphore_signal(barrier, inc=1, device_id=peer, device_id_type=MESH)
    own.wait()

    def pack(h):
        for t in range(packs):
            low, high = out[t, :, pl.ds(128 * h, 128)], out[t + packs, :, pl.ds(128 * h, 128)]
            for c in (0, 1):
                lanes = slice(64 * c, 64 * c + 64)
                panels[2 * h + c][row * packs + t] = jnp.concatenate([low[:, lanes], high[:, lanes]], axis=1)

    pack(0)
    pl.semaphore_wait(barrier, len(peers))

    def piece(h, spot):
        dy, dz, up = spot
        return panels[h].at[pl.ds(at_row(dy, dz) * packs + up * half, half)]

    def ring_copies(h):
        copies = []
        for target, spots in ((up_y, FORWARD), (down_y, BACKWARD), (other_z, ACROSS)):
            for spot in spots:
                k = len(copies)
                copies.append(
                    pltpu.make_async_remote_copy(
                        piece(h, spot), piece(h, spot), ring_send.at[h, k], ring_recv.at[h, k],
                        device_id=target, device_id_type=MESH,
                    )
                )
        return copies

    def twin_copies(h):
        return [
            pltpu.make_async_remote_copy(
                piece(h, spot), piece(h, spot), twin_send.at[h, k], twin_recv.at[h, k],
                device_id=twin, device_id_type=MESH,
            )
            for k, spot in enumerate(LANDED + ((0, 0, 0), (0, 0, 1)))
        ]

    ring = [ring_copies(h) for h in range(CHUNKS)]
    sibling = [twin_copies(h) for h in range(CHUNKS)]

    def gather_start(h):
        for k in (0, 5, 10, 1, 6, 11):
            ring[h][k].start()
        sibling[h][14].start()
        sibling[h][15].start()

    def gather_step(h, k, then=()):
        ring[h][k].wait_recv()
        for k_next in then:
            ring[h][k_next].start()
        sibling[h][k].start()

    def gather_first(h):
        gather_step(h, 10, (2,))
        gather_step(h, 0, (3, 12))
        gather_step(h, 5, (8, 13))

    def gather_more(h):
        gather_step(h, 11, (7,))
        gather_step(h, 1)
        gather_step(h, 6)

    def gather_second(h):
        following = ring[h + 1] if h + 1 < CHUNKS else None
        if following:
            following[10].start()
            following[11].start()
        gather_step(h, 2, (4,))
        if following:
            following[0].start()
            following[1].start()
        gather_step(h, 7, (9,))
        if following:
            following[5].start()
            following[6].start()
            sibling[h + 1][14].start()
            sibling[h + 1][15].start()

    def gather_rest(h):
        for k in (12, 13, 3, 8, 4, 9):
            gather_step(h, k)
        for copy in sibling[h]:
            copy.wait_recv()

    def products(h, low, high, total):
        panel = panels[h]

        def body(i, total):
            for j in range(UNROLL):
                s = i * UNROLL + j
                left = jnp.concatenate([tile_store[slot[2 * s]], tile_store[slot[2 * s + 1]]], axis=1)
                right = jnp.concatenate(
                    [panel[col[2 * s + e]] * sides[side[2 * s + e]] for e in (0, 1)], axis=0
                )
                total = total * keep[s] + jnp.dot(left, right, preferred_element_type=jnp.float32)
                sums[s] = (total + pltpu.roll(total, 64, 1)).astype(jnp.bfloat16)
            return total

        return lax.fori_loop(low // UNROLL, high // UNROLL, body, total)

    def collect(h):
        part, base = parts[h]

        def body(q, carry):
            for t in range(packs):
                r = q * block + t
                part[base + q * packs + t] = sums[last[r]] * sides[0] + sums[last[r + packs]] * sides[1]
            return carry

        lax.fori_loop(0, X * ZH, body, 0)

    def spot(h, dx, dz, up):
        return pl.ds(parts[h][1] + at_column(dx, dz) * packs + up * half, half)

    def sum_copies(h):
        copies = []
        for dz in (1, 0):
            for target, spots in (
                (up_x, ((2, dz, 0), (1, dz, 1), (1, dz, 0))),
                (down_x, ((2, dz, 1), (-1, dz, 0), (-1, dz, 1))),
            ):
                copies += [(target, s) for s in spots]
        copies += [(far_z, (0, 1, 0)), (far_z, (0, 1, 1))]
        return [
            pltpu.make_async_remote_copy(
                parts[h][0].at[spot(h, *s)], gots[h].at[k], sum_send.at[h, k], sum_recv.at[h, k],
                device_id=target, device_id_type=MESH,
            )
            for k, (target, s) in enumerate(copies)
        ]

    adds = [sum_copies(h) for h in range(CHUNKS)]

    def wide(value):
        return value.astype(jnp.float32)

    def sum_start(h, i):
        for k in (0, 3, 1, 4):
            adds[h][6 * i + k].start()

    def sum_pass(h, i):
        part, got, dz = parts[h][0], gots[h], 1 - i
        for k, dx, up, k_next in ((0, 1, 0, 2), (3, -1, 1, 5)):
            adds[h][6 * i + k].wait_recv()
            here = spot(h, dx, dz, up)
            part[here] = (wide(part[here]) + wide(got[6 * i + k])).astype(jnp.bfloat16)
            adds[h][6 * i + k_next].start()

    def sum_across(h):
        part, got = parts[h][0], gots[h]
        for up, ks in ((0, (2, 4)), (1, (1, 5))):
            for k in ks:
                adds[h][k].wait_recv()
            here = spot(h, 0, 1, up)
            part[here] = (wide(part[here]) + wide(got[ks[0]]) + wide(got[ks[1]])).astype(jnp.bfloat16)
            adds[h][12 + up].start()

    def sum_end(h):
        part, got = parts[h][0], gots[h]
        for up, ks in ((1, (7, 11, 13)), (0, (8, 10, 12))):
            for k in ks:
                adds[h][k].wait_recv()
            total = wide(part[spot(h, 0, 0, up)])
            for k in ks:
                total = total + wide(got[k])
            total = total.astype(jnp.bfloat16)
            if h % 2 == 0:
                agg[pl.ds(up * half, half)] = total
            else:
                lanes = pl.ds(128 * (h // 2), 128)
                for t in range(half):
                    before, now = agg[up * half + t], total[t]
                    out[up * half + t, :, lanes] = jnp.concatenate([before[:, :64], now[:, :64]], axis=1)
                    out[packs + up * half + t, :, lanes] = jnp.concatenate([before[:, 64:], now[:, 64:]], axis=1)

    gather_start(0)
    group = slots // tile_sem.shape[0]
    tile_loads = [
        pltpu.make_async_copy(
            tiles.at[pl.ds(i * group, group)], tile_store.at[pl.ds(i * group, group)], tile_sem.at[i]
        )
        for i in range(tile_sem.shape[0])
    ]
    for copy in tile_loads:
        copy.start()
    pack(1)
    zero = jnp.zeros((128, 128), jnp.float32)
    tile_store[slots] = zero.astype(jnp.bfloat16)
    sums[pairs] = zero.astype(jnp.bfloat16)
    lane = lax.broadcasted_iota(jnp.int32, (1, 128), 1)
    sides[0] = jnp.where(lane < 64, 1.0, 0.0).astype(jnp.bfloat16)
    sides[1] = jnp.where(lane < 64, 0.0, 1.0).astype(jnp.bfloat16)
    gather_first(0)
    gather_more(0)
    gather_second(0)
    quarter, end = pairs // 4, CHUNKS - 1
    for h in range(CHUNKS):
        gather_rest(h)
        if h == 0:
            for copy in tile_loads:
                copy.wait()
        if h > 0:
            sum_pass(h - 1, 0)
        total = products(h, 0, quarter, zero)
        if h < end:
            gather_first(h + 1)
        total = products(h, quarter, 2 * quarter, total)
        if h < end:
            gather_more(h + 1)
        total = products(h, 2 * quarter, 3 * quarter, total)
        if h > 0:
            sum_pass(h - 1, 1)
        products(h, 3 * quarter, pairs, total)
        if h > 1:
            for copy in ring[h - 2] + sibling[h - 2]:
                copy.wait_send()
        collect(h)
        sum_start(h, 0)
        if h < end:
            sum_start(h, 1)
            gather_second(h + 1)
        if h > 0:
            sum_across(h - 1)
        if h > 1:
            sum_end(h - 2)
    sum_pass(end, 0)
    sum_start(end, 1)
    sum_end(end - 1)
    sum_across(end)
    sum_pass(end, 1)
    sum_end(end)
    for copy in sum(ring[2:] + sibling[2:] + adds, []):
        copy.wait_send()


def on_device(features, tiles, tile_rows, tile_cols, valid, weight, bias):
    sub_rows, width = features.shape
    size, slots = tiles.shape[3], tiles.shape[2]
    block = sub_rows // size
    row_tiles = block * X * ZH
    packs = block // 2
    pairs = (slots // 2 + row_tiles) // 2
    slot, col, side, keep, last = tables(
        tile_rows[0, 0], tile_cols[0, 0], valid[0, 0], row_tiles, pairs, block
    )
    smem, vmem = pl.BlockSpec(memory_space=pltpu.SMEM), pl.BlockSpec(memory_space=pltpu.VMEM)
    hbm = pl.BlockSpec(memory_space=pl.ANY)
    dma = pltpu.SemaphoreType.DMA

    def store(*shape):
        return pltpu.VMEM(shape + (size, size), jnp.bfloat16)

    aggregated = pl.pallas_call(
        functools.partial(kernel, slots, pairs, row_tiles, block),
        name="graph_layer",
        out_shape=jax.ShapeDtypeStruct((block, size, width), jnp.bfloat16),
        in_specs=[smem, smem, smem, smem, smem, hbm, hbm],
        out_specs=vmem,
        scratch_shapes=[
            store(slots + 1),
            *[store(packs * Y * ZL * CORE)] * CHUNKS,
            store(pairs + 1),
            store(row_tiles),
            *[store(14, packs // 2)] * CHUNKS,
            store(packs),
            pltpu.VMEM((2, 1, size), jnp.bfloat16),
            dma, dma((8,)), *[dma((CHUNKS, 14))] * 2, *[dma((CHUNKS, 16))] * 2, *[dma((CHUNKS, 14))] * 2,
        ],
        compiler_params=pltpu.CompilerParams(
            collective_id=0, has_side_effects=True, vmem_limit_bytes=67043328
        ),
    )(
        slot, col, side, keep, last,
        features.reshape(block, size, width), tiles.reshape(slots, size, size),
    )
    mixed = jnp.dot(aggregated.reshape(sub_rows, width), weight, preferred_element_type=jnp.float32) + bias
    return jnp.maximum(mixed, 0.0).astype(jnp.bfloat16)


def solution(mesh):
    return jax.shard_map(
        on_device,
        mesh=mesh,
        in_specs=(
            P(("row", "col"), None),
            P("row", "col", None, None, None),
            P("row", "col", None),
            P("row", "col", None),
            P("row", "col", None),
            P(),
            P(),
        ),
        out_specs=P(("row", "col"), None),
        check_vma=False,
    )
```

```python
import functools

import jax
import jax.numpy as jnp
from jax import lax
from jax.experimental import pallas as pl
from jax.experimental.pallas import tpu as pltpu
from jax.sharding import PartitionSpec as P

MESH = pl.DeviceIdType.MESH
Y, ZL, CORE, X, ZH = 4, 2, 2, 4, 2
CHUNKS = 4
UNROLL = 16
FORWARD = ((0, 0, 0), (0, 0, 1), (0, 1, 1), (-1, 0, 0), (-1, 1, 1))
BACKWARD = ((0, 0, 1), (0, 0, 0), (0, 1, 0), (1, 0, 1), (1, 1, 0))
ACROSS = ((0, 0, 1), (0, 0, 0), (-1, 0, 0), (1, 0, 1))
LANDED = (
    tuple((dy - 1, dz, up) for dy, dz, up in FORWARD)
    + tuple((dy + 1, dz, up) for dy, dz, up in BACKWARD)
    + tuple((dy, 1 - dz, up) for dy, dz, up in ACROSS)
)


def tables(rows, cols, valid, code_ref, keep_ref, last_ref, row_tiles, pairs, block):
    slots, width, packs = rows.shape[1], row_tiles, block // 2
    span = 2 * packs * Y * ZL * CORE

    def iota(shape, axis):
        return lax.broadcasted_iota(jnp.int32, shape, axis)

    square = (width, width)
    eye = iota(square, 0) == iota(square, 1)
    row_ids = iota(square, 1)

    def upright(line):
        return jnp.sum(jnp.where(eye, line, 0), axis=1, keepdims=True)

    key = jnp.where(valid > 0, rows, row_tiles)
    place_in_panel = ((cols // block) * packs + cols % packs) * 2 + (cols % block) // packs
    keys, codes, ranks = [], [], []
    count = jnp.zeros((1, width), jnp.int32)
    for b in range(slots // width):
        lanes = slice(b * width, (b + 1) * width)
        keys.append(upright(key[:, lanes]))
        ids = b * width + iota((width, 1), 0)
        codes.append((ids - slots) * span + upright(place_in_panel[:, lanes]))
        earlier = (keys[b] == key) & (iota((width, slots), 1) < ids)
        ranks.append(jnp.sum(earlier.astype(jnp.int32), axis=1, keepdims=True))
        count += jnp.sum((keys[b] == row_ids).astype(jnp.int32), axis=0, keepdims=True)
    used = (count + 1) >> 1
    start = jnp.sum(jnp.where(iota(square, 0) < row_ids, upright(used), 0), axis=0, keepdims=True)
    code = jnp.full((1, 2 * pairs), slots * span, jnp.int32)
    order = iota((width, 2 * pairs), 1)
    for b in range(slots // width):
        at = ranks[b] + 2 * jnp.sum(jnp.where(keys[b] == row_ids, start, 0), axis=1, keepdims=True)
        at = jnp.where(keys[b] < row_tiles, at, -1)
        code += jnp.sum(jnp.where(at == order, codes[b], 0), axis=0, keepdims=True)
    code_ref[...] = code
    first = upright(jnp.where(count > 0, start, -1)) == iota((width, pairs), 1)
    keep_ref[...] = 1.0 - jnp.sum(first.astype(jnp.float32), axis=0, keepdims=True)
    last_ref[...] = jnp.where(count > 0, start + used - 1, pairs)


def kernel(
    slots, pairs, row_tiles, block,
    rows, cols, valid, features, tiles, out,
    tile_store, panel_0, panel_1, panel_2, panel_3, sums, part_a, got_0, got_1, got_2, got_3, agg, sides,
    code_line, keep_line, last_line, code, keep, last, table_sem, own_sem, tile_sem, ring_send, ring_recv, twin_send, twin_recv, sum_send, sum_recv,
):
    packs = block // 2
    half = packs // 2
    span = 2 * packs * Y * ZL * CORE
    shift = span.bit_length() - 1
    row, column = lax.axis_index("row"), lax.axis_index("col")
    zl, y, core = row // (Y * CORE), (row // CORE) % Y, row % CORE
    x, zh = column // ZH, column % ZH

    def at_row(dy, dz, dc=0):
        return ((zl + dz) % ZL) * (Y * CORE) + ((y + dy + Y) % Y) * CORE + (core + dc) % CORE

    def at_column(dx, dz):
        return ((x + dx + X) % X) * ZH + (zh + dz) % ZH

    up_y, down_y = (at_row(1, 0), column), (at_row(-1, 0), column)
    other_z, twin = (at_row(0, 1), column), (at_row(0, 0, 1), column)
    up_x, down_x = (row, at_column(1, 0)), (row, at_column(-1, 0))
    far_z = (row, at_column(0, 1))

    panels, gots = (panel_0, panel_1, panel_2, panel_3), (got_0, got_1, got_2, got_3)
    parts = ((part_a, 0), (part_a, row_tiles // 2), (panel_0, 0), (panel_1, 0))

    own = pltpu.make_async_copy(features, out, own_sem)
    own.start()
    barrier = pltpu.get_barrier_semaphore()
    peers = (up_y, down_y, other_z, twin, up_x, down_x, far_z)
    for peer in peers:
        pl.semaphore_signal(barrier, inc=1, device_id=peer, device_id_type=MESH)
    own.wait()

    def pack(h):
        for t in range(packs):
            low, high = out[t, :, pl.ds(128 * h, 128)], out[t + packs, :, pl.ds(128 * h, 128)]
            for c in (0, 1):
                lanes = slice(64 * c, 64 * c + 64)
                panels[2 * h + c][row * packs + t] = jnp.concatenate([low[:, lanes], high[:, lanes]], axis=1)

    pack(0)
    pl.semaphore_wait(barrier, len(peers))

    def piece(h, spot):
        dy, dz, up = spot
        return panels[h].at[pl.ds(at_row(dy, dz) * packs + up * half, half)]

    def ring_copies(h):
        copies = []
        for target, spots in ((up_y, FORWARD), (down_y, BACKWARD), (other_z, ACROSS)):
            for spot in spots:
                k = len(copies)
                copies.append(
                    pltpu.make_async_remote_copy(
                        piece(h, spot), piece(h, spot), ring_send.at[h, k], ring_recv.at[h, k],
                        device_id=target, device_id_type=MESH,
                    )
                )
        return copies

    def twin_copies(h):
        return [
            pltpu.make_async_remote_copy(
                piece(h, spot), piece(h, spot), twin_send.at[h, k], twin_recv.at[h, k],
                device_id=twin, device_id_type=MESH,
            )
            for k, spot in enumerate(LANDED + ((0, 0, 0), (0, 0, 1)))
        ]

    ring = [ring_copies(h) for h in range(CHUNKS)]
    sibling = [twin_copies(h) for h in range(CHUNKS)]

    def gather_start(h):
        for k in (0, 5, 10, 1, 6, 11):
            ring[h][k].start()
        sibling[h][14].start()
        sibling[h][15].start()

    def gather_step(h, k, then=()):
        ring[h][k].wait_recv()
        for k_next in then:
            ring[h][k_next].start()
        sibling[h][k].start()

    def gather_first(h):
        gather_step(h, 10, (2,))
        gather_step(h, 0, (3, 12))
        gather_step(h, 5, (8, 13))

    def gather_more(h):
        gather_step(h, 11, (7,))
        gather_step(h, 1)
        gather_step(h, 6)

    def gather_second(h):
        following = ring[h + 1] if h + 1 < CHUNKS else None
        if following:
            following[10].start()
            following[11].start()
        gather_step(h, 2, (4,))
        if following:
            following[0].start()
            following[1].start()
        gather_step(h, 7, (9,))
        if following:
            following[5].start()
            following[6].start()
            sibling[h + 1][14].start()
            sibling[h + 1][15].start()

    def gather_rest(h):
        for k in (12, 13, 3, 8, 4, 9):
            gather_step(h, k)
        for copy in sibling[h]:
            copy.wait_recv()

    def products(h, low, high, total):
        panel = panels[h]

        def body(i, total):
            for j in range(UNROLL):
                s = i * UNROLL + j
                pair = [code[0, 2 * s], code[0, 2 * s + 1]]
                left = jnp.concatenate([tile_store[c >> shift] for c in pair], axis=1)
                right = jnp.concatenate([panel[(c & (span - 1)) >> 1] * sides[c & 1] for c in pair], axis=0)
                total = total * keep[0, s] + jnp.dot(left, right, preferred_element_type=jnp.float32)
                sums[s] = (total + pltpu.roll(total, 64, 1)).astype(jnp.bfloat16)
            return total

        return lax.fori_loop(low // UNROLL, high // UNROLL, body, total)

    def collect(h):
        part, base = parts[h]

        def body(q, carry):
            for t in range(packs):
                r = q * block + t
                part[base + q * packs + t] = sums[last[0, r]] * sides[0] + sums[last[0, r + packs]] * sides[1]
            return carry

        lax.fori_loop(0, X * ZH, body, 0)

    def spot(h, dx, dz, up):
        return pl.ds(parts[h][1] + at_column(dx, dz) * packs + up * half, half)

    def sum_copies(h):
        copies = []
        for dz in (1, 0):
            for target, spots in (
                (up_x, ((2, dz, 0), (1, dz, 1), (1, dz, 0))),
                (down_x, ((2, dz, 1), (-1, dz, 0), (-1, dz, 1))),
            ):
                copies += [(target, s) for s in spots]
        copies += [(far_z, (0, 1, 0)), (far_z, (0, 1, 1))]
        return [
            pltpu.make_async_remote_copy(
                parts[h][0].at[spot(h, *s)], gots[h].at[k], sum_send.at[h, k], sum_recv.at[h, k],
                device_id=target, device_id_type=MESH,
            )
            for k, (target, s) in enumerate(copies)
        ]

    adds = [sum_copies(h) for h in range(CHUNKS)]

    def wide(value):
        return value.astype(jnp.float32)

    def sum_start(h, i):
        for k in (0, 3, 1, 4):
            adds[h][6 * i + k].start()

    def sum_pass(h, i):
        part, got, dz = parts[h][0], gots[h], 1 - i
        for k, dx, up, k_next in ((0, 1, 0, 2), (3, -1, 1, 5)):
            adds[h][6 * i + k].wait_recv()
            here = spot(h, dx, dz, up)
            part[here] = (wide(part[here]) + wide(got[6 * i + k])).astype(jnp.bfloat16)
            adds[h][6 * i + k_next].start()

    def sum_across(h):
        part, got = parts[h][0], gots[h]
        for up, ks in ((0, (2, 4)), (1, (1, 5))):
            for k in ks:
                adds[h][k].wait_recv()
            here = spot(h, 0, 1, up)
            part[here] = (wide(part[here]) + wide(got[ks[0]]) + wide(got[ks[1]])).astype(jnp.bfloat16)
            adds[h][12 + up].start()

    def sum_end(h):
        part, got = parts[h][0], gots[h]
        for up, ks in ((1, (7, 11, 13)), (0, (8, 10, 12))):
            for k in ks:
                adds[h][k].wait_recv()
            total = wide(part[spot(h, 0, 0, up)])
            for k in ks:
                total = total + wide(got[k])
            total = total.astype(jnp.bfloat16)
            if h % 2 == 0:
                agg[pl.ds(up * half, half)] = total
            else:
                lanes = pl.ds(128 * (h // 2), 128)
                for t in range(half):
                    before, now = agg[up * half + t], total[t]
                    out[up * half + t, :, lanes] = jnp.concatenate([before[:, :64], now[:, :64]], axis=1)
                    out[packs + up * half + t, :, lanes] = jnp.concatenate([before[:, 64:], now[:, 64:]], axis=1)

    gather_start(0)
    group = slots // tile_sem.shape[0]
    tile_loads = [
        pltpu.make_async_copy(
            tiles.at[pl.ds(i * group, group)], tile_store.at[pl.ds(i * group, group)], tile_sem.at[i]
        )
        for i in range(tile_sem.shape[0])
    ]
    for copy in tile_loads:
        copy.start()
    pack(1)
    zero = jnp.zeros((128, 128), jnp.float32)
    tile_store[slots] = zero.astype(jnp.bfloat16)
    sums[pairs] = zero.astype(jnp.bfloat16)
    lane = lax.broadcasted_iota(jnp.int32, (1, 128), 1)
    sides[0] = jnp.where(lane < 64, 1.0, 0.0).astype(jnp.bfloat16)
    sides[1] = jnp.where(lane < 64, 0.0, 1.0).astype(jnp.bfloat16)
    tables(rows[...], cols[...], valid[...], code_line, keep_line, last_line, row_tiles, pairs, block)
    table_loads = [
        pltpu.make_async_copy(line, table, table_sem.at[i])
        for i, (line, table) in enumerate(((code_line, code), (keep_line, keep), (last_line, last)))
    ]
    gather_first(0)
    for copy in table_loads:
        copy.start()
    gather_more(0)
    gather_second(0)
    quarter, end = pairs // 4, CHUNKS - 1
    for h in range(CHUNKS):
        gather_rest(h)
        if h == 0:
            for copy in tile_loads + table_loads:
                copy.wait()
        if h > 0:
            sum_pass(h - 1, 0)
        total = products(h, 0, quarter, zero)
        if h < end:
            gather_first(h + 1)
        total = products(h, quarter, 2 * quarter, total)
        if h < end:
            gather_more(h + 1)
        total = products(h, 2 * quarter, 3 * quarter, total)
        if h > 0:
            sum_pass(h - 1, 1)
        products(h, 3 * quarter, pairs, total)
        if h > 1:
            for copy in ring[h - 2] + sibling[h - 2]:
                copy.wait_send()
        collect(h)
        sum_start(h, 0)
        if h < end:
            sum_start(h, 1)
            gather_second(h + 1)
        if h > 0:
            sum_across(h - 1)
        if h > 1:
            sum_end(h - 2)
    sum_pass(end, 0)
    sum_start(end, 1)
    sum_end(end - 1)
    sum_across(end)
    sum_pass(end, 1)
    sum_end(end)
    for copy in sum(ring[2:] + sibling[2:] + adds, []):
        copy.wait_send()


def on_device(features, tiles, tile_rows, tile_cols, valid, weight, bias):
    sub_rows, width = features.shape
    size, slots = tiles.shape[3], tiles.shape[2]
    block = sub_rows // size
    row_tiles = block * X * ZH
    packs = block // 2
    pairs = (slots // 2 + row_tiles) // 2
    vmem, hbm = pl.BlockSpec(memory_space=pltpu.VMEM), pl.BlockSpec(memory_space=pl.ANY)
    dma = pltpu.SemaphoreType.DMA

    def store(*shape):
        return pltpu.VMEM(shape + (size, size), jnp.bfloat16)

    aggregated = pl.pallas_call(
        functools.partial(kernel, slots, pairs, row_tiles, block),
        name="graph_layer",
        out_shape=jax.ShapeDtypeStruct((block, size, width), jnp.bfloat16),
        in_specs=[vmem, vmem, vmem, hbm, hbm],
        out_specs=vmem,
        scratch_shapes=[
            store(slots + 1),
            *[store(packs * Y * ZL * CORE)] * CHUNKS,
            store(pairs + 1),
            store(row_tiles),
            *[store(14, packs // 2)] * CHUNKS,
            store(packs),
            pltpu.VMEM((2, 1, size), jnp.bfloat16),
            pltpu.VMEM((1, 2 * pairs), jnp.int32), pltpu.VMEM((1, pairs), jnp.float32), pltpu.VMEM((1, row_tiles), jnp.int32),
            pltpu.SMEM((1, 2 * pairs), jnp.int32), pltpu.SMEM((1, pairs), jnp.float32), pltpu.SMEM((1, row_tiles), jnp.int32),
            dma((3,)), dma, dma((8,)), *[dma((CHUNKS, 14))] * 2, *[dma((CHUNKS, 16))] * 2, *[dma((CHUNKS, 14))] * 2,
        ],
        compiler_params=pltpu.CompilerParams(
            collective_id=0, has_side_effects=True, vmem_limit_bytes=67043328
        ),
    )(
        tile_rows[0], tile_cols[0], valid[0],
        features.reshape(block, size, width), tiles.reshape(slots, size, size),
    )
    mixed = jnp.dot(aggregated.reshape(sub_rows, width), weight, preferred_element_type=jnp.float32) + bias
    return jnp.maximum(mixed, 0.0).astype(jnp.bfloat16)


def solution(mesh):
    return jax.shard_map(
        on_device,
        mesh=mesh,
        in_specs=(
            P(("row", "col"), None),
            P("row", "col", None, None, None),
            P("row", "col", None),
            P("row", "col", None),
            P("row", "col", None),
            P(),
            P(),
        ),
        out_specs=P(("row", "col"), None),
        check_vma=False,
    )
```

```python
import functools

import jax
import jax.numpy as jnp
from jax import lax
from jax.experimental import pallas as pl
from jax.experimental.pallas import tpu as pltpu
from jax.sharding import PartitionSpec as P

MESH = pl.DeviceIdType.MESH
Y, ZL, CORE, X, ZH = 4, 2, 2, 4, 2
CHUNKS = 4
UNROLL = 32
FORWARD = ((0, 0, 0), (0, 0, 1), (0, 1, 1), (-1, 0, 0), (-1, 1, 1))
BACKWARD = ((0, 0, 1), (0, 0, 0), (0, 1, 0), (1, 0, 1), (1, 1, 0))
ACROSS = ((0, 0, 1), (0, 0, 0), (-1, 0, 0), (1, 0, 1))
LANDED = (
    tuple((dy - 1, dz, up) for dy, dz, up in FORWARD)
    + tuple((dy + 1, dz, up) for dy, dz, up in BACKWARD)
    + tuple((dy, 1 - dz, up) for dy, dz, up in ACROSS)
)


def tables(rows, cols, valid, code_ref, keep_ref, last_ref, row_tiles, pairs, block):
    slots, width, packs = rows.shape[1], row_tiles, block // 2
    span = 2 * packs * Y * ZL * CORE

    def iota(shape, axis):
        return lax.broadcasted_iota(jnp.int32, shape, axis)

    square = (width, width)
    eye = iota(square, 0) == iota(square, 1)
    row_ids = iota(square, 1)

    def upright(line):
        return jnp.sum(jnp.where(eye, line, 0), axis=1, keepdims=True)

    key = jnp.where(valid > 0, rows, row_tiles)
    place_in_panel = ((cols // block) * packs + cols % packs) * 2 + (cols % block) // packs
    keys, codes, ranks = [], [], []
    count = jnp.zeros((1, width), jnp.int32)
    for b in range(slots // width):
        lanes = slice(b * width, (b + 1) * width)
        keys.append(upright(key[:, lanes]))
        ids = b * width + iota((width, 1), 0)
        codes.append((ids - slots) * span + upright(place_in_panel[:, lanes]))
        earlier = (keys[b] == key) & (iota((width, slots), 1) < ids)
        ranks.append(jnp.sum(earlier.astype(jnp.int32), axis=1, keepdims=True))
        count += jnp.sum((keys[b] == row_ids).astype(jnp.int32), axis=0, keepdims=True)
    used = (count + 1) >> 1
    start = jnp.sum(jnp.where(iota(square, 0) < row_ids, upright(used), 0), axis=0, keepdims=True)
    code = jnp.full((1, 2 * pairs), slots * span, jnp.int32)
    order = iota((width, 2 * pairs), 1)
    for b in range(slots // width):
        at = ranks[b] + 2 * jnp.sum(jnp.where(keys[b] == row_ids, start, 0), axis=1, keepdims=True)
        at = jnp.where(keys[b] < row_tiles, at, -1)
        code += jnp.sum(jnp.where(at == order, codes[b], 0), axis=0, keepdims=True)
    code_ref[...] = code
    first = upright(jnp.where(count > 0, start, -1)) == iota((width, pairs), 1)
    keep_ref[...] = 1.0 - jnp.sum(first.astype(jnp.float32), axis=0, keepdims=True)
    last_ref[...] = jnp.where(count > 0, start + used - 1, pairs)


def kernel(
    slots, pairs, row_tiles, block,
    rows, cols, valid, features, tiles, out,
    tile_store, panel_0, panel_1, panel_2, panel_3, sums, part_a, got_0, got_1, got_2, got_3, agg, sides,
    code_line, keep_line, last_line, code, keep, last, table_sem, own_sem, tile_sem, ring_send, ring_recv, twin_send, twin_recv, sum_send, sum_recv,
):
    packs = block // 2
    half = packs // 2
    span = 2 * packs * Y * ZL * CORE
    shift = span.bit_length() - 1
    row, column = lax.axis_index("row"), lax.axis_index("col")
    zl, y, core = row // (Y * CORE), (row // CORE) % Y, row % CORE
    x, zh = column // ZH, column % ZH

    def at_row(dy, dz, dc=0):
        return ((zl + dz) % ZL) * (Y * CORE) + ((y + dy + Y) % Y) * CORE + (core + dc) % CORE

    def at_column(dx, dz):
        return ((x + dx + X) % X) * ZH + (zh + dz) % ZH

    up_y, down_y = (at_row(1, 0), column), (at_row(-1, 0), column)
    other_z, twin = (at_row(0, 1), column), (at_row(0, 0, 1), column)
    up_x, down_x = (row, at_column(1, 0)), (row, at_column(-1, 0))
    far_z = (row, at_column(0, 1))

    panels, gots = (panel_0, panel_1, panel_2, panel_3), (got_0, got_1, got_2, got_3)
    parts = ((part_a, 0), (part_a, row_tiles // 2), (panel_0, 0), (panel_1, 0))

    own = pltpu.make_async_copy(features, out, own_sem)
    own.start()
    barrier = pltpu.get_barrier_semaphore()
    peers = (up_y, down_y, other_z, twin, up_x, down_x, far_z)
    for peer in peers:
        pl.semaphore_signal(barrier, inc=1, device_id=peer, device_id_type=MESH)
    own.wait()

    def pack(h):
        for t in range(packs):
            low, high = out[t, :, pl.ds(128 * h, 128)], out[t + packs, :, pl.ds(128 * h, 128)]
            for c in (0, 1):
                lanes = slice(64 * c, 64 * c + 64)
                panels[2 * h + c][row * packs + t] = jnp.concatenate([low[:, lanes], high[:, lanes]], axis=1)

    pack(0)
    pl.semaphore_wait(barrier, len(peers))

    def piece(h, spot):
        dy, dz, up = spot
        return panels[h].at[pl.ds(at_row(dy, dz) * packs + up * half, half)]

    def ring_copies(h):
        copies = []
        for target, spots in ((up_y, FORWARD), (down_y, BACKWARD), (other_z, ACROSS)):
            for spot in spots:
                k = len(copies)
                copies.append(
                    pltpu.make_async_remote_copy(
                        piece(h, spot), piece(h, spot), ring_send.at[h], ring_recv.at[h, k],
                        device_id=target, device_id_type=MESH,
                    )
                )
        return copies

    def twin_copies(h):
        return [
            pltpu.make_async_remote_copy(
                piece(h, spot), piece(h, spot), twin_send.at[h], twin_recv.at[h],
                device_id=twin, device_id_type=MESH,
            )
            for k, spot in enumerate(LANDED + ((0, 0, 0), (0, 0, 1)))
        ]

    def whole(pieces, send, recv):
        ref = panel_2.at[pl.ds(0, pieces * half)]
        return pltpu.make_async_remote_copy(ref, ref, send, recv, device_id=twin, device_id_type=MESH)

    def gather_sent(h):
        whole(14, ring_send.at[h], ring_recv.at[h, 0]).wait_send()
        whole(16, twin_send.at[h], twin_recv.at[h]).wait_send()

    ring = [ring_copies(h) for h in range(CHUNKS)]
    sibling = [twin_copies(h) for h in range(CHUNKS)]

    def gather_start(h):
        for k in (0, 5, 10, 1, 6, 11):
            ring[h][k].start()
        sibling[h][14].start()
        sibling[h][15].start()

    def gather_step(h, k, then=()):
        ring[h][k].wait_recv()
        for k_next in then:
            ring[h][k_next].start()
        sibling[h][k].start()

    def gather_first(h):
        gather_step(h, 10, (2,))
        gather_step(h, 0, (3, 12))
        gather_step(h, 5, (8, 13))

    def gather_more(h):
        gather_step(h, 11, (7,))
        gather_step(h, 1)
        gather_step(h, 6)

    def gather_second(h):
        following = ring[h + 1] if h + 1 < CHUNKS else None
        if following:
            following[10].start()
            following[11].start()
        gather_step(h, 2, (4,))
        if following:
            following[0].start()
            following[1].start()
        gather_step(h, 7, (9,))
        if following:
            following[5].start()
            following[6].start()
            sibling[h + 1][14].start()
            sibling[h + 1][15].start()

    def gather_rest(h):
        for k in (12, 13, 3, 8, 4, 9):
            gather_step(h, k)
        whole(16, twin_send.at[h], twin_recv.at[h]).wait_recv()

    def products(h, low, high, total):
        panel, unroll = panels[h], UNROLL

        def body(i, total):
            for j in range(unroll):
                s = i * unroll + j
                pair = [code[0, 2 * s], code[0, 2 * s + 1]]
                left = jnp.concatenate([tile_store[c >> shift] for c in pair], axis=1)
                right = jnp.concatenate([panel[(c & (span - 1)) >> 1] * sides[c & 1] for c in pair], axis=0)
                total = total * keep[0, s] + jnp.dot(left, right, preferred_element_type=jnp.float32)
                sums[s] = (total + pltpu.roll(total, 64, 1)).astype(jnp.bfloat16)
            return total

        return lax.fori_loop(low // unroll, high // unroll, body, total)

    def collect(h):
        part, base = parts[h]
        order = ((2, 1), (1, 1), (-1, 1), (2, 0), (1, 0), (-1, 0), (0, 1), (0, 0))
        ready = {0: (0, 3), 1: (1,), 2: (4,)}
        if h < CHUNKS - 1:
            ready |= {3: (6, 9), 4: (7,), 5: (10,)}
        for i, (dx, dz) in enumerate(order):
            q = at_column(dx, dz)
            for t in range(packs):
                r = q * block + t
                part[base + q * packs + t] = sums[last[0, r]] * sides[0] + sums[last[0, r + packs]] * sides[1]
            for k in ready.get(i, ()):
                adds[h][k].start()

    def spot(h, dx, dz, up):
        return pl.ds(parts[h][1] + at_column(dx, dz) * packs + up * half, half)

    def sum_copies(h):
        copies = []
        for dz in (1, 0):
            for target, spots in (
                (up_x, ((2, dz, 0), (1, dz, 1), (1, dz, 0))),
                (down_x, ((2, dz, 1), (-1, dz, 0), (-1, dz, 1))),
            ):
                copies += [(target, s) for s in spots]
        copies += [(far_z, (0, 1, 0)), (far_z, (0, 1, 1))]
        return [
            pltpu.make_async_remote_copy(
                parts[h][0].at[spot(h, *s)], gots[h].at[k], sum_send.at[h], sum_recv.at[h, k],
                device_id=target, device_id_type=MESH,
            )
            for k, (target, s) in enumerate(copies)
        ]

    adds = [sum_copies(h) for h in range(CHUNKS)]

    def wide(value):
        return value.astype(jnp.float32)

    def sum_start(h, i):
        for k in (0, 3, 1, 4):
            adds[h][6 * i + k].start()

    def sum_pass(h, i):
        part, got, dz = parts[h][0], gots[h], 1 - i
        for k, dx, up, k_next in ((0, 1, 0, 2), (3, -1, 1, 5)):
            adds[h][6 * i + k].wait_recv()
            here = spot(h, dx, dz, up)
            part[here] = (wide(part[here]) + wide(got[6 * i + k])).astype(jnp.bfloat16)
            adds[h][6 * i + k_next].start()

    def sum_across(h):
        part, got = parts[h][0], gots[h]
        for up, ks in ((0, (2, 4)), (1, (1, 5))):
            for k in ks:
                adds[h][k].wait_recv()
            here = spot(h, 0, 1, up)
            part[here] = (wide(part[here]) + wide(got[ks[0]]) + wide(got[ks[1]])).astype(jnp.bfloat16)
            adds[h][12 + up].start()

    def sum_end(h):
        part, got = parts[h][0], gots[h]
        for up, ks in ((1, (7, 11, 13)), (0, (8, 10, 12))):
            for k in ks:
                adds[h][k].wait_recv()
            total = wide(part[spot(h, 0, 0, up)])
            for k in ks:
                total = total + wide(got[k])
            total = total.astype(jnp.bfloat16)
            if h % 2 == 0:
                agg[pl.ds(up * half, half)] = total
            else:
                lanes = pl.ds(128 * (h // 2), 128)
                for t in range(half):
                    before, now = agg[up * half + t], total[t]
                    out[up * half + t, :, lanes] = jnp.concatenate([before[:, :64], now[:, :64]], axis=1)
                    out[packs + up * half + t, :, lanes] = jnp.concatenate([before[:, 64:], now[:, 64:]], axis=1)

    gather_start(0)
    group = slots // tile_sem.shape[0]
    tile_loads = [
        pltpu.make_async_copy(
            tiles.at[pl.ds(i * group, group)], tile_store.at[pl.ds(i * group, group)], tile_sem.at[i]
        )
        for i in range(tile_sem.shape[0])
    ]
    for copy in tile_loads:
        copy.start()
    pack(1)
    zero = jnp.zeros((128, 128), jnp.float32)
    tile_store[slots] = zero.astype(jnp.bfloat16)
    sums[pairs] = zero.astype(jnp.bfloat16)
    lane = lax.broadcasted_iota(jnp.int32, (1, 128), 1)
    sides[0] = jnp.where(lane < 64, 1.0, 0.0).astype(jnp.bfloat16)
    sides[1] = jnp.where(lane < 64, 0.0, 1.0).astype(jnp.bfloat16)
    tables(rows[...], cols[...], valid[...], code_line, keep_line, last_line, row_tiles, pairs, block)
    table_loads = [
        pltpu.make_async_copy(line, table, table_sem.at[i])
        for i, (line, table) in enumerate(((code_line, code), (keep_line, keep), (last_line, last)))
    ]
    gather_first(0)
    for copy in table_loads:
        copy.start()
    gather_more(0)
    gather_second(0)
    quarter, end = pairs // 4, CHUNKS - 1
    for h in range(CHUNKS):
        gather_rest(h)
        if h == 0:
            for copy in tile_loads + table_loads:
                copy.wait()
        if h > 0:
            sum_pass(h - 1, 0)
        total = products(h, 0, quarter, zero)
        if h < end:
            gather_first(h + 1)
        total = products(h, quarter, 2 * quarter, total)
        if h < end:
            gather_more(h + 1)
        total = products(h, 2 * quarter, 3 * quarter, total)
        if h > 0:
            sum_pass(h - 1, 1)
        products(h, 3 * quarter, pairs, total)
        if h > 1:
            gather_sent(h - 2)
        collect(h)
        if h < end:
            gather_second(h + 1)
        if h > 0:
            sum_across(h - 1)
        if h > 1:
            sum_end(h - 2)
    sum_pass(end, 0)
    sum_start(end, 1)
    sum_end(end - 1)
    sum_across(end)
    sum_pass(end, 1)
    sum_end(end)
    for h in range(CHUNKS):
        if h > 1:
            gather_sent(h)
        whole(14, sum_send.at[h], sum_recv.at[h, 0]).wait_send()


def on_device(features, tiles, tile_rows, tile_cols, valid, weight, bias):
    sub_rows, width = features.shape
    size, slots = tiles.shape[3], tiles.shape[2]
    block = sub_rows // size
    row_tiles = block * X * ZH
    packs = block // 2
    pairs = (slots // 2 + row_tiles) // 2
    vmem, hbm = pl.BlockSpec(memory_space=pltpu.VMEM), pl.BlockSpec(memory_space=pl.ANY)
    dma = pltpu.SemaphoreType.DMA

    def store(*shape):
        return pltpu.VMEM(shape + (size, size), jnp.bfloat16)

    aggregated = pl.pallas_call(
        functools.partial(kernel, slots, pairs, row_tiles, block),
        name="graph_layer",
        out_shape=jax.ShapeDtypeStruct((block, size, width), jnp.bfloat16),
        in_specs=[vmem, vmem, vmem, hbm, hbm],
        out_specs=vmem,
        scratch_shapes=[
            store(slots + 1),
            *[store(packs * Y * ZL * CORE)] * CHUNKS,
            store(pairs + 1),
            store(row_tiles),
            *[store(14, packs // 2)] * CHUNKS,
            store(packs),
            pltpu.VMEM((2, 1, size), jnp.bfloat16),
            pltpu.VMEM((1, 2 * pairs), jnp.int32), pltpu.VMEM((1, pairs), jnp.float32), pltpu.VMEM((1, row_tiles), jnp.int32),
            pltpu.SMEM((1, 2 * pairs), jnp.int32), pltpu.SMEM((1, pairs), jnp.float32), pltpu.SMEM((1, row_tiles), jnp.int32),
            dma((3,)), dma, dma((8,)), dma((CHUNKS,)), dma((CHUNKS, 14)), dma((CHUNKS,)), dma((CHUNKS,)), dma((CHUNKS,)), dma((CHUNKS, 14)),
        ],
        compiler_params=pltpu.CompilerParams(
            collective_id=0, has_side_effects=True, vmem_limit_bytes=67043328
        ),
    )(
        tile_rows[0], tile_cols[0], valid[0],
        features.reshape(block, size, width), tiles.reshape(slots, size, size),
    )
    mixed = jnp.dot(aggregated.reshape(sub_rows, width), weight, preferred_element_type=jnp.float32) + bias
    return jnp.maximum(mixed, 0.0).astype(jnp.bfloat16)


def solution(mesh):
    return jax.shard_map(
        on_device,
        mesh=mesh,
        in_specs=(
            P(("row", "col"), None),
            P("row", "col", None, None, None),
            P("row", "col", None),
            P("row", "col", None),
            P("row", "col", None),
            P(),
            P(),
        ),
        out_specs=P(("row", "col"), None),
        check_vma=False,
    )
```

```python
import functools

import jax
import jax.numpy as jnp
from jax import lax
from jax.experimental import pallas as pl
from jax.experimental.pallas import tpu as pltpu
from jax.sharding import PartitionSpec as P

MESH = pl.DeviceIdType.MESH
Y, ZL, CORE, X, ZH = 4, 2, 2, 4, 2
CHUNKS = 4
UNROLL = 32
FORWARD = ((0, 0, 0), (0, 0, 1), (0, 1, 1), (-1, 0, 0), (-1, 1, 1))
BACKWARD = ((0, 0, 1), (0, 0, 0), (0, 1, 0), (1, 0, 1), (1, 1, 0))
ACROSS = ((0, 0, 1), (0, 0, 0), (-1, 0, 0), (1, 0, 1))
LANDED = (
    tuple((dy - 1, dz, up) for dy, dz, up in FORWARD)
    + tuple((dy + 1, dz, up) for dy, dz, up in BACKWARD)
    + tuple((dy, 1 - dz, up) for dy, dz, up in ACROSS)
)


def tables(rows, cols, valid, code_ref, keep_ref, last_ref, row_tiles, pairs, block):
    slots, width, packs = rows.shape[1], row_tiles, block // 2
    span = 2 * packs * Y * ZL * CORE

    def iota(shape, axis):
        return lax.broadcasted_iota(jnp.int32, shape, axis)

    square = (width, width)
    eye = iota(square, 0) == iota(square, 1)
    row_ids = iota(square, 1)

    def upright(line):
        return jnp.sum(jnp.where(eye, line, 0), axis=1, keepdims=True)

    key = jnp.where(valid > 0, rows, row_tiles)
    place_in_panel = ((cols // block) * packs + cols % packs) * 2 + (cols % block) // packs
    keys, codes, ranks = [], [], []
    count = jnp.zeros((1, width), jnp.int32)
    for b in range(slots // width):
        lanes = slice(b * width, (b + 1) * width)
        keys.append(upright(key[:, lanes]))
        ids = b * width + iota((width, 1), 0)
        codes.append((ids - slots) * span + upright(place_in_panel[:, lanes]))
        earlier = (keys[b] == key) & (iota((width, slots), 1) < ids)
        ranks.append(jnp.sum(earlier.astype(jnp.int32), axis=1, keepdims=True))
        count += jnp.sum((keys[b] == row_ids).astype(jnp.int32), axis=0, keepdims=True)
    used = (count + 1) >> 1
    start = jnp.sum(jnp.where(iota(square, 0) < row_ids, upright(used), 0), axis=0, keepdims=True)
    code = jnp.full((1, 2 * pairs), slots * span, jnp.int32)
    order = iota((width, 2 * pairs), 1)
    for b in range(slots // width):
        at = ranks[b] + 2 * jnp.sum(jnp.where(keys[b] == row_ids, start, 0), axis=1, keepdims=True)
        at = jnp.where(keys[b] < row_tiles, at, -1)
        code += jnp.sum(jnp.where(at == order, codes[b], 0), axis=0, keepdims=True)
    code_ref[...] = code
    first = upright(jnp.where(count > 0, start, -1)) == iota((width, pairs), 1)
    keep_ref[...] = 1.0 - jnp.sum(first.astype(jnp.float32), axis=0, keepdims=True)
    last_ref[...] = jnp.where(count > 0, start + used - 1, pairs)


def kernel(
    slots, pairs, row_tiles, block,
    rows, cols, valid, features, tiles, out,
    tile_store, panel_0, panel_1, panel_2, panel_3, sums, part_a, got_0, got_1, got_2, got_3, agg, sides,
    code_line, keep_line, last_line, code, keep, last, table_sem, own_sem, tile_sem, ring_send, ring_recv, twin_send, twin_recv, sum_send, sum_recv,
):
    packs = block // 2
    half = packs // 2
    span = 2 * packs * Y * ZL * CORE
    shift = span.bit_length() - 1
    row, column = lax.axis_index("row"), lax.axis_index("col")
    zl, y, core = row // (Y * CORE), (row // CORE) % Y, row % CORE
    x, zh = column // ZH, column % ZH

    def at_row(dy, dz, dc=0):
        return ((zl + dz) % ZL) * (Y * CORE) + ((y + dy + Y) % Y) * CORE + (core + dc) % CORE

    def at_column(dx, dz):
        return ((x + dx + X) % X) * ZH + (zh + dz) % ZH

    up_y, down_y = (at_row(1, 0), column), (at_row(-1, 0), column)
    other_z, twin = (at_row(0, 1), column), (at_row(0, 0, 1), column)
    up_x, down_x = (row, at_column(1, 0)), (row, at_column(-1, 0))
    far_z = (row, at_column(0, 1))

    panels, gots = (panel_0, panel_1, panel_2, panel_3), (got_0, got_1, got_2, got_3)
    parts = ((part_a, 0), (part_a, row_tiles // 2), (panel_0, 0), (panel_1, 0))

    own = pltpu.make_async_copy(features, out, own_sem)
    own.start()
    barrier = pltpu.get_barrier_semaphore()
    peers = (up_y, down_y, other_z, twin, up_x, down_x, far_z)
    for peer in peers:
        pl.semaphore_signal(barrier, inc=1, device_id=peer, device_id_type=MESH)
    own.wait()

    def pack(h):
        for t in range(packs):
            low, high = out[t, :, pl.ds(128 * h, 128)], out[t + packs, :, pl.ds(128 * h, 128)]
            for c in (0, 1):
                lanes = slice(64 * c, 64 * c + 64)
                panels[2 * h + c][row * packs + t] = jnp.concatenate([low[:, lanes], high[:, lanes]], axis=1)

    pack(0)
    pl.semaphore_wait(barrier, len(peers))

    def piece(h, spot):
        dy, dz, up = spot
        return panels[h].at[pl.ds(at_row(dy, dz) * packs + up * half, half)]

    def ring_copies(h):
        copies = []
        for target, spots in ((up_y, FORWARD), (down_y, BACKWARD), (other_z, ACROSS)):
            for spot in spots:
                k = len(copies)
                copies.append(
                    pltpu.make_async_remote_copy(
                        piece(h, spot), piece(h, spot), ring_send.at[h], ring_recv.at[h, k],
                        device_id=target, device_id_type=MESH,
                    )
                )
        return copies

    def twin_copies(h):
        return [
            pltpu.make_async_remote_copy(
                piece(h, spot), piece(h, spot), twin_send.at[h], twin_recv.at[h],
                device_id=twin, device_id_type=MESH,
            )
            for k, spot in enumerate(LANDED + ((0, 0, 0), (0, 0, 1)))
        ]

    def whole(pieces, send, recv):
        ref = panel_2.at[pl.ds(0, pieces * half)]
        return pltpu.make_async_remote_copy(ref, ref, send, recv, device_id=twin, device_id_type=MESH)

    def gather_sent(h):
        whole(14, ring_send.at[h], ring_recv.at[h, 0]).wait_send()
        whole(16, twin_send.at[h], twin_recv.at[h]).wait_send()

    ring = [ring_copies(h) for h in range(CHUNKS)]
    sibling = [twin_copies(h) for h in range(CHUNKS)]

    def gather_start(h):
        for k in (0, 5, 10, 1, 6, 11):
            ring[h][k].start()
        sibling[h][14].start()
        sibling[h][15].start()

    def gather_step(h, k, then=()):
        ring[h][k].wait_recv()
        for k_next in then:
            ring[h][k_next].start()
        sibling[h][k].start()

    def gather_first(h):
        gather_step(h, 10, (2,))
        gather_step(h, 0, (3, 12))
        gather_step(h, 5, (8, 13))

    def gather_more(h):
        gather_step(h, 11, (7,))
        gather_step(h, 1)
        gather_step(h, 6)

    def gather_second(h):
        following = ring[h + 1] if h + 1 < CHUNKS else None
        if following:
            following[10].start()
            following[11].start()
        gather_step(h, 2, (4,))
        if following:
            following[0].start()
            following[1].start()
        gather_step(h, 7, (9,))
        if following:
            following[5].start()
            following[6].start()
            sibling[h + 1][14].start()
            sibling[h + 1][15].start()

    def gather_rest(h):
        for k in (12, 13, 3, 8, 4, 9):
            gather_step(h, k)
        whole(16, twin_send.at[h], twin_recv.at[h]).wait_recv()

    def products(h, low, high, total):
        panel, unroll = panels[h], UNROLL

        def body(i, total):
            for j in range(unroll):
                s = i * unroll + j
                pair = [code[0, 2 * s], code[0, 2 * s + 1]]
                left = jnp.concatenate([tile_store[c >> shift] for c in pair], axis=1)
                right = jnp.concatenate([panel[(c & (span - 1)) >> 1] * sides[c & 1] for c in pair], axis=0)
                total = total * keep[0, s] + jnp.dot(left, right, preferred_element_type=jnp.float32)
                sums[s] = (total + pltpu.roll(total, 64, 1)).astype(jnp.bfloat16)
            return total

        return lax.fori_loop(low // unroll, high // unroll, body, total)

    def collect(h):
        part, base = parts[h]
        order = ((2, 1), (1, 1), (-1, 1), (2, 0), (1, 0), (-1, 0), (0, 1), (0, 0))
        ready = {0: (0, 3), 1: (1,), 2: (4,)}
        if h < CHUNKS - 1:
            ready |= {3: (6, 9), 4: (7,), 5: (10,)}
        for i, (dx, dz) in enumerate(order):
            q = at_column(dx, dz)
            for t in range(packs):
                r = q * block + t
                part[base + q * packs + t] = sums[last[0, r]] * sides[0] + sums[last[0, r + packs]] * sides[1]
            for k in ready.get(i, ()):
                adds[h][k].start()

    def spot(h, dx, dz, up):
        return pl.ds(parts[h][1] + at_column(dx, dz) * packs + up * half, half)

    def sum_copies(h):
        copies = []
        for dz in (1, 0):
            for target, spots in (
                (up_x, ((2, dz, 0), (1, dz, 1), (1, dz, 0))),
                (down_x, ((2, dz, 1), (-1, dz, 0), (-1, dz, 1))),
            ):
                copies += [(target, s) for s in spots]
        copies += [(far_z, (0, 1, 0)), (far_z, (0, 1, 1))]
        return [
            pltpu.make_async_remote_copy(
                parts[h][0].at[spot(h, *s)], gots[h].at[k], sum_send.at[h], sum_recv.at[h, k],
                device_id=target, device_id_type=MESH,
            )
            for k, (target, s) in enumerate(copies)
        ]

    adds = [sum_copies(h) for h in range(CHUNKS)]

    def wide(value):
        return value.astype(jnp.float32)

    def sum_start(h, i):
        for k in (0, 3, 1, 4):
            adds[h][6 * i + k].start()

    def sum_pass(h, i):
        part, got, dz = parts[h][0], gots[h], 1 - i
        for k, dx, up, k_next in ((0, 1, 0, 2), (3, -1, 1, 5)):
            adds[h][6 * i + k].wait_recv()
            here = spot(h, dx, dz, up)
            part[here] = (wide(part[here]) + wide(got[6 * i + k])).astype(jnp.bfloat16)
            adds[h][6 * i + k_next].start()

    def sum_across(h):
        part, got = parts[h][0], gots[h]
        for up, ks in ((0, (2, 4)), (1, (1, 5))):
            for k in ks:
                adds[h][k].wait_recv()
            here = spot(h, 0, 1, up)
            part[here] = (wide(part[here]) + wide(got[ks[0]]) + wide(got[ks[1]])).astype(jnp.bfloat16)
            adds[h][12 + up].start()

    def sum_end(h):
        part, got = parts[h][0], gots[h]
        for up, ks in ((1, (7, 11, 13)), (0, (8, 10, 12))):
            for k in ks:
                adds[h][k].wait_recv()
            total = wide(part[spot(h, 0, 0, up)])
            for k in ks:
                total = total + wide(got[k])
            total = total.astype(jnp.bfloat16)
            if h % 2 == 0:
                agg[pl.ds(up * half, half)] = total
            else:
                lanes = pl.ds(128 * (h // 2), 128)
                for t in range(half):
                    before, now = agg[up * half + t], total[t]
                    out[up * half + t, :, lanes] = jnp.concatenate([before[:, :64], now[:, :64]], axis=1)
                    out[packs + up * half + t, :, lanes] = jnp.concatenate([before[:, 64:], now[:, 64:]], axis=1)

    gather_start(0)
    group = slots // tile_sem.shape[0]
    tile_loads = [
        pltpu.make_async_copy(
            tiles.at[pl.ds(i * group, group)], tile_store.at[pl.ds(i * group, group)], tile_sem.at[i]
        )
        for i in range(tile_sem.shape[0])
    ]
    for copy in tile_loads:
        copy.start()
    pack(1)
    zero = jnp.zeros((128, 128), jnp.float32)
    tile_store[slots] = zero.astype(jnp.bfloat16)
    sums[pairs] = zero.astype(jnp.bfloat16)
    lane = lax.broadcasted_iota(jnp.int32, (1, 128), 1)
    sides[0] = jnp.where(lane < 64, 1.0, 0.0).astype(jnp.bfloat16)
    sides[1] = jnp.where(lane < 64, 0.0, 1.0).astype(jnp.bfloat16)
    tables(rows[...], cols[...], valid[...], code_line, keep_line, last_line, row_tiles, pairs, block)
    table_loads = [
        pltpu.make_async_copy(line, table, table_sem.at[i])
        for i, (line, table) in enumerate(((code_line, code), (keep_line, keep), (last_line, last)))
    ]
    gather_first(0)
    for copy in table_loads:
        copy.start()
    gather_more(0)
    gather_second(0)
    quarter, end = pairs // 4, CHUNKS - 1
    for h in range(CHUNKS):
        gather_rest(h)
        if h == 0:
            for copy in tile_loads + table_loads:
                copy.wait()
        if h > 0:
            sum_pass(h - 1, 0)
        total = products(h, 0, quarter, zero)
        if h < end:
            gather_first(h + 1)
        total = products(h, quarter, 2 * quarter, total)
        if h < end:
            gather_more(h + 1)
        total = products(h, 2 * quarter, 3 * quarter, total)
        if h > 0:
            sum_pass(h - 1, 1)
        products(h, 3 * quarter, pairs, total)
        if h > 1:
            gather_sent(h - 2)
        collect(h)
        if h < end:
            gather_second(h + 1)
        if h > 0:
            sum_across(h - 1)
        if h > 1:
            sum_end(h - 2)
    sum_pass(end, 0)
    sum_start(end, 1)
    sum_end(end - 1)
    sum_across(end)
    sum_pass(end, 1)
    sum_end(end)
    for h in range(CHUNKS):
        if h > 1:
            gather_sent(h)
        whole(14, sum_send.at[h], sum_recv.at[h, 0]).wait_send()


def on_device(features, tiles, tile_rows, tile_cols, valid, weight, bias):
    sub_rows, width = features.shape
    size, slots = tiles.shape[3], tiles.shape[2]
    block = sub_rows // size
    row_tiles = block * X * ZH
    packs = block // 2
    pairs = (slots // 2 + row_tiles) // 2
    vmem, hbm = pl.BlockSpec(memory_space=pltpu.VMEM), pl.BlockSpec(memory_space=pl.ANY)
    dma = pltpu.SemaphoreType.DMA

    def store(*shape):
        return pltpu.VMEM(shape + (size, size), jnp.bfloat16)

    aggregated = pl.pallas_call(
        functools.partial(kernel, slots, pairs, row_tiles, block),
        name="graph_layer",
        out_shape=pltpu.VMEM((block, size, width), jnp.bfloat16),
        in_specs=[vmem, vmem, vmem, hbm, hbm],
        out_specs=vmem,
        scratch_shapes=[
            store(slots + 1),
            *[store(packs * Y * ZL * CORE)] * CHUNKS,
            store(pairs + 1),
            store(row_tiles),
            *[store(14, packs // 2)] * CHUNKS,
            store(packs),
            pltpu.VMEM((2, 1, size), jnp.bfloat16),
            pltpu.VMEM((1, 2 * pairs), jnp.int32), pltpu.VMEM((1, pairs), jnp.float32), pltpu.VMEM((1, row_tiles), jnp.int32),
            pltpu.SMEM((1, 2 * pairs), jnp.int32), pltpu.SMEM((1, pairs), jnp.float32), pltpu.SMEM((1, row_tiles), jnp.int32),
            dma((3,)), dma, dma((8,)), dma((CHUNKS,)), dma((CHUNKS, 14)), dma((CHUNKS,)), dma((CHUNKS,)), dma((CHUNKS,)), dma((CHUNKS, 14)),
        ],
        compiler_params=pltpu.CompilerParams(
            collective_id=0, has_side_effects=True, vmem_limit_bytes=65500000
        ),
    )(
        tile_rows[0], tile_cols[0], valid[0],
        features.reshape(block, size, width), tiles.reshape(slots, size, size),
    )
    mixed = jnp.dot(aggregated.reshape(sub_rows, width), weight, preferred_element_type=jnp.float32) + bias
    return jnp.maximum(mixed, 0.0).astype(jnp.bfloat16)


def solution(mesh):
    return jax.shard_map(
        on_device,
        mesh=mesh,
        in_specs=(
            P(("row", "col"), None),
            P("row", "col", None, None, None),
            P("row", "col", None),
            P("row", "col", None),
            P("row", "col", None),
            P(),
            P(),
        ),
        out_specs=P(("row", "col"), None),
        check_vma=False,
    )
```
